256 devices in a mesh: rep: 16 (over x_lo, y, core), fsdp: 16 (over z, x_hi).
Axes of the slice: x: 4 (x_hi: 2, x_lo: 2; x = x_hi * 2 + x_lo), y: 4, z: 8, core: 2. Of those that a mesh axis runs over, the one named last changes fastest.
Arguments:
- latents: float32 [2, 256, 320, 256], P(None, ('rep', 'fsdp')), may hold values from -6 to 6
- gaussian: float32 [2, 256, 320, 256], P(None, ('rep', 'fsdp')), may hold values from -6 to 6
- stamps: int32 [2, 256], P(None, ('rep', 'fsdp')), may hold values from 0 to 999
- numerator: float32 [16, 320, 2880], P('rep', 'fsdp'), may hold values from -6 to 6
- momentum: float32 [16, 320, 2880], P('rep', 'fsdp'), may hold values from -1.5 to 1.5
- push_weight: float32 [16], P('rep'), may hold values from 0.5 to 2
- arrived_numerator: float32 [16, 320, 2880], P('rep', 'fsdp'), may hold values from -6 to 6
- arrived_weight: float32 [16], P('rep'), may hold values from 0.25 to 1
Outputs:
- numerator_out: float32 [16, 320, 2880], P('rep', 'fsdp')
- momentum_out: float32 [16, 320, 2880], P('rep', 'fsdp')
- weight_out: float32 [16], P('rep')
- pending_numerator: float32 [16, 320, 2880], P('rep', 'fsdp')
- pending_weight: float32 [16], P('rep')
The draws below stay inside these ranges and needn't reach their ends.
All inputs are finite; a program needn't handle non-finite values.
Results may differ from the reference program's by a relative error of at most 0.0003.
Values sent between devices are 32-bit elements; how exact they have to be, the bound alone decides.
No kernel may reach another device: no remote copies, remote signals or barrier semaphores. Data moves between devices by JAX's collectives and lax.ppermute only.
A program may use at most 64 MiB of HBM per device.

```python
import math
import jax
import jax.numpy as jnp
from jax import lax

C = 320
GROUPS = 32
CROP_H = 16
CROP_W = 16
STEPS = 2
TRAIN_T = 1000
PIX = 256
KKC = 2880
REPS = 16
BATCH = 256


def touch_ends(array, stream_key, smallest, largest):
    longest = array.shape.index(max(array.shape))
    spots = []
    for shift in (0, 1):
        where = [jax.random.randint(jax.random.fold_in(stream_key, axis), (), 0, length) for axis, length in enumerate(array.shape)]
        where[longest] = (where[longest] + shift) % array.shape[longest]
        spots.append(tuple(where))
    return array.at[spots[0]].set(smallest).at[spots[1]].set(largest)


def block_scale(rng, shape, pieces, low, top_value):
    def one(dim, shards_of):
        steps = jax.random.uniform(jax.random.fold_in(jax.random.fold_in(rng, 6), dim), (shards_of,), jnp.float32, low / len(pieces), top_value / len(pieces))
        return jnp.repeat(jnp.exp(steps), shape[dim] // shards_of).reshape((-1,) + (1,) * (len(shape) - dim - 1))

    factor_of = one(*pieces[0])
    for cut in pieces[1:]:
        factor_of = factor_of * one(*cut)
    return factor_of


def noise(rng, extent, width, bound, cuts=(), kind=jnp.bfloat16):
    array = width * jax.random.normal(rng, extent, jnp.float32)
    if cuts:
        array = array * block_scale(rng, extent, cuts, -0.22, 0.18)
    return jnp.clip(array, -bound, bound).astype(kind)


def setup_inputs(seed: int = 0) -> dict:
    keys = jax.random.split(jax.random.key(seed), 9)
    return {
        "latents": noise(keys[0], (STEPS, BATCH, C, PIX), 1.0, 6.0, ((1, 256),), jnp.float32),
        "gaussian": noise(keys[1], (STEPS, BATCH, C, PIX), 1.0, 6.0, ((1, 256),), jnp.float32),
        "stamps": touch_ends(jax.random.randint(keys[2], (STEPS, BATCH), 0, TRAIN_T), jax.random.fold_in(keys[2], 1), 0, TRAIN_T - 1).astype(jnp.int32),
        "numerator": noise(keys[3], (REPS, C, KKC), 1.0, 6.0, ((0, 16), (1, 16)), jnp.float32),
        "momentum": noise(keys[4], (REPS, C, KKC), 0.1, 1.5, ((0, 16), (1, 16)), jnp.float32),
        "push_weight": jnp.clip(jnp.exp(math.log(2.0) - 1.3862944 * jax.random.uniform(keys[5], (REPS,), jnp.float32) ** block_scale(keys[5], (REPS,), ((0, 16),), -0.2, 0.2)), 0.5, 2.0),
        "arrived_numerator": noise(keys[6], (REPS, C, KKC), 0.5, 6.0, ((0, 16), (1, 16)), jnp.float32),
        "arrived_weight": jnp.clip(jnp.exp(math.log(1.0) - 1.3862944 * jax.random.uniform(keys[7], (REPS,), jnp.float32) ** block_scale(keys[7], (REPS,), ((0, 16),), -0.2, 0.2)), 0.25, 1.0),
    }


norm_epsilon = 1e-05
momentum_decay = 0.9
step_size = 1.0
beta_first = 0.00085
beta_last = 0.012
highest = lax.Precision.HIGHEST

def noise_levels(stamps):
    fraction = jnp.arange(TRAIN_T, dtype=jnp.float32) / (TRAIN_T - 1)
    root_first = beta_first ** 0.5
    root_last = beta_last ** 0.5
    beta_values = jnp.square(root_first + fraction * (root_last - root_first))
    cumulative = jnp.cumprod(1.0 - beta_values)
    matches = stamps[..., None] == jnp.arange(TRAIN_T, dtype=jnp.int32)
    return lax.optimization_barrier(jnp.sum(jnp.where(matches, cumulative, jnp.float32(0.0)), axis=-1))

def activations(latents, gaussian, stamps):
    levels = noise_levels(stamps)[:, None, None]
    noised = jnp.sqrt(levels) * latents + jnp.sqrt(1.0 - levels) * gaussian
    samples, channels, pixels = noised.shape
    grouped = noised.reshape(samples, GROUPS, channels // GROUPS, pixels)
    center = lax.optimization_barrier(jnp.mean(grouped, axis=(2, 3), keepdims=True))
    spread = lax.optimization_barrier(jnp.mean(jnp.square(grouped - center), axis=(2, 3), keepdims=True))
    normed = ((grouped - center) * lax.rsqrt(spread + norm_epsilon)).reshape(samples, channels, pixels)
    return (jax.nn.silu(normed), noised - gaussian)

def unfold_taps(signal):
    samples, channels, pixels = signal.shape
    picture = signal.reshape(samples, channels, CROP_H, CROP_W)
    padded = jnp.pad(picture, ((0, 0), (0, 0), (1, 1), (1, 1)))
    shifted = [padded[:, :, row_shift:row_shift + CROP_H, col_shift:col_shift + CROP_W] for row_shift in range(3) for col_shift in range(3)]
    return jnp.stack(shifted, axis=1).reshape(samples, 9 * channels, pixels)

def replica_gradient(kernel, latents, gaussian, stamps):
    hidden_acts, target_gap = activations(latents, gaussian, stamps)
    unfolded = unfold_taps(hidden_acts)
    tap_scale = kernel.shape[1] ** (-0.5)
    output = jnp.einsum('oj,bjp->bop', kernel, unfolded, precision=highest)
    residual = target_gap + tap_scale * output
    summed = jnp.einsum('bop,bjp->oj', residual, unfolded, precision=highest)
    return summed * (tap_scale / latents.shape[0])

def reference(latents, gaussian, stamps, numerator, momentum, push_weight, arrived_numerator, arrived_weight):
    replicas = numerator.shape[0]
    per_replica = latents.shape[1] // replicas
    split_latents = latents.reshape(latents.shape[0], replicas, per_replica, latents.shape[2], latents.shape[3])
    split_gaussian = gaussian.reshape(gaussian.shape[0], replicas, per_replica, gaussian.shape[2], gaussian.shape[3])
    split_stamps = stamps.reshape(stamps.shape[0], replicas, per_replica)

    def one_replica(bundle):
        return replica_gradient(bundle[0], bundle[1], bundle[2], bundle[3])
    for step_index in range(STEPS):
        kernel = numerator / push_weight[:, None, None]
        gradient = lax.map(one_replica, (kernel, split_latents[step_index], split_gaussian[step_index], split_stamps[step_index]))
        momentum = momentum_decay * momentum + gradient
        moved = numerator - step_size * momentum
        numerator = 0.5 * moved + arrived_numerator
        sent_weight = 0.5 * push_weight
        push_weight = sent_weight + arrived_weight
        distance = 2 ** step_index
        arrived_numerator = jnp.roll(0.5 * moved, distance, axis=0)
        arrived_weight = jnp.roll(sent_weight, distance, axis=0)
    return (numerator, momentum, push_weight, arrived_numerator, arrived_weight)
```

```python
import functools
import math

import numpy as np
import jax
import jax.numpy as jnp
from jax import lax
from jax.experimental import pallas as pl
from jax.experimental.pallas import tpu as pltpu
from jax.sharding import Mesh
from jax.sharding import PartitionSpec as P


C = 320
GROUP = 10
SIDE = 16
PIX = 256
TAPS = 9
STEPS = 2
TRAIN_T = 1000
KKC = 2880
Z = 8
OWN = 20
PAIR = 40
HALF = 160
BATCH = 16

norm_epsilon = 1e-05
momentum_decay = 0.9
step_size = 1.0
beta_first = 0.00085
beta_last = 0.012

VMEM = pl.BlockSpec(memory_space=pltpu.VMEM)
SMEM = pl.BlockSpec(memory_space=pltpu.SMEM)


def level_table():
    fraction = np.arange(TRAIN_T, dtype=np.float64) / (TRAIN_T - 1)
    first, last = beta_first**0.5, beta_last**0.5
    levels = np.cumprod(1.0 - np.square(first + fraction * (last - first)))
    table = np.zeros(1024, np.float32)
    table[:TRAIN_T] = levels.astype(np.float32)
    return table.reshape(8, 128)


def tap_offset(tap):
    return (tap // 3 - 1, tap % 3 - 1)


def tap_mask(tap, rows):
    pixel = lax.broadcasted_iota(jnp.int32, (rows, PIX), 1)
    row, column = pixel >> 4, pixel & 15
    down, right = tap_offset(tap)
    ok = None
    if down:
        ok = (row + down >= 0) & (row + down < SIDE)
    if right:
        side = (column + right >= 0) & (column + right < SIDE)
        ok = side if ok is None else ok & side
    return ok


def split_bf16(value):
    high = value.astype(jnp.bfloat16)
    low = (value - high.astype(jnp.float32)).astype(jnp.bfloat16)
    return high, low


def prepare_kernel(step, z_ref, stamps_ref, table_ref, lat_ref, gau_ref, up0, dn0, up1, dn1, own_t, gap):
    stamp = stamps_ref[step, 0]
    spot = lax.broadcasted_iota(jnp.int32, (8, 128), 0) * 128 + lax.broadcasted_iota(
        jnp.int32, (8, 128), 1
    )
    level = jnp.sum(jnp.where(spot == stamp, table_ref[...], 0.0), axis=(0, 1), keepdims=True)
    gaussian = gau_ref[0, 0]
    noised = jnp.sqrt(level) * lat_ref[0, 0] + jnp.sqrt(1.0 - level) * gaussian
    gap[...] = noised - gaussian

    row_group = (lax.broadcasted_iota(jnp.int32, (C, C), 0) * 205) >> 11
    col_group = (lax.broadcasted_iota(jnp.int32, (C, C), 1) * 205) >> 11
    same = jnp.where(row_group == col_group, 1.0, 0.0).astype(jnp.float32)

    def group_mean(value):
        sums = jnp.broadcast_to(jnp.sum(value, axis=1, keepdims=True), (C, 128))
        mixed = jnp.dot(
            same, sums, precision=lax.Precision.HIGHEST, preferred_element_type=jnp.float32
        )
        return mixed[:, :1] * (1.0 / (GROUP * PIX))

    centered = noised - group_mean(noised)
    normed = centered * lax.rsqrt(group_mean(centered * centered) + norm_epsilon)
    hidden = normed / (1.0 + jnp.exp(-normed))
    up0[:HALF] = hidden[:HALF]
    dn0[:HALF] = hidden[:HALF]
    up1[:HALF] = hidden[HALF:]
    dn1[:HALF] = hidden[HALF:]

    z = z_ref[0]

    def rows_of(distance, start, count):
        first = lax.rem(z + distance + Z, Z) * PAIR + start
        return gap[pl.ds(pl.multiple_of(first, 8), count), :]

    for hop in (1, 2, 3):
        at = HALF + PAIR * (hop - 1)
        up1[at : at + PAIR] = rows_of(hop, 0, PAIR)
        dn0[at : at + PAIR] = rows_of(-hop, 0, PAIR)
    up0[HALF : HALF + 24] = rows_of(4, 0, 24)
    dn1[HALF : HALF + 16] = rows_of(4, 24, 16)
    own_t[...] = rows_of(0, 0, PAIR)


def prepare(step, z_index, stamps, table, latents, gaussian):
    pick = pl.BlockSpec((1, 1, C, PIX), lambda i: (step, 0, 0, 0))
    whole = lambda rows: pl.BlockSpec((rows, PIX), lambda i: (0, 0))
    sizes = (HALF + 24, HALF + 120, HALF + 120, HALF + 16, PAIR)
    return pl.pallas_call(
        functools.partial(prepare_kernel, step),
        grid=(1,),
        in_specs=[SMEM, SMEM, pl.BlockSpec((8, 128), lambda i: (0, 0)), pick, pick],
        out_specs=[whole(rows) for rows in sizes],
        out_shape=[jax.ShapeDtypeStruct((rows, PIX), jnp.float32) for rows in sizes],
        scratch_shapes=[pltpu.VMEM((C, PIX), jnp.float32)],
        cost_estimate=pl.CostEstimate(
            flops=200_000_000, bytes_accessed=2_000_000, transcendentals=82_000
        ),
        name="prepare",
    )(z_index, stamps, table, latents, gaussian)


def gradient_kernel(
    x_ref, own_k, pair_k, own_up0, own_up1, own_t, *rest
):
    up0, rest = rest[:4], rest[4:]
    dn0, rest = rest[:3], rest[3:]
    up1, rest = rest[:3], rest[3:]
    dn1, rest = rest[:4], rest[4:]
    keep, send, both, taps, shifted, h_high, h_low, r_high, r_low = rest
    x = x_ref[0]

    @pl.when(x == 0)
    def _():
        both[:OWN] = own_k[...]
        both[OWN:] = pair_k[...]

    @pl.when(x != 0)
    def _():
        both[:OWN] = pair_k[...]
        both[OWN:] = own_k[...]

    for tap in range(TAPS):
        taps[PAIR * tap : PAIR * (tap + 1)] = both[:, C * tap : C * (tap + 1)]
    k_high, k_low = split_bf16(taps[...])
    scale = KKC**-0.5
    masks = [tap_mask(tap, PAIR) for tap in range(TAPS)]

    def dot(a, b):
        return jnp.dot(a, b, preferred_element_type=jnp.float32)

    samples = [(own_up0, own_up1, lambda: own_t[...])]
    for hop in (1, 2, 3):
        at = HALF + PAIR * (hop - 1)
        samples.append(
            (up0[hop - 1], up1[hop - 1], lambda r=up1[hop - 1], at=at: r[at : at + PAIR])
        )
        samples.append(
            (dn0[hop - 1], dn1[hop - 1], lambda r=dn0[hop - 1], at=at: r[at : at + PAIR])
        )
    samples.append(
        (
            up0[3],
            dn1[3],
            lambda: jnp.concatenate([up0[3][HALF : HALF + 24], dn1[3][HALF : HALF + 16]], axis=0),
        )
    )
    for index, (first, second, gap) in enumerate(samples):
        lanes = slice(PIX * index, PIX * (index + 1))
        hidden = jnp.concatenate([first[:HALF], second[:HALF]], axis=0)
        high, low = split_bf16(hidden)
        h_high[:, lanes] = high
        h_low[:, lanes] = low
        product = dot(k_high, high) + dot(k_high, low) + dot(k_low, high)
        output = product[4 * PAIR : 5 * PAIR]
        for tap in range(TAPS):
            if tap == 4:
                continue
            down, right = tap_offset(tap)
            moved = pltpu.roll(
                product[PAIR * tap : PAIR * (tap + 1)], (-(SIDE * down + right)) % PIX, 1
            )
            output = output + jnp.where(masks[tap], moved, 0.0)
        residual = gap() + scale * output
        for tap in range(TAPS):
            down, right = tap_offset(tap)
            value = residual
            if tap != 4:
                value = pltpu.roll(
                    jnp.where(masks[tap], residual, 0.0), (SIDE * down + right) % PIX, 1
                )
            shifted[PAIR * tap : PAIR * (tap + 1)] = value
        high, low = split_bf16(shifted[...])
        r_high[:, lanes] = high
        r_low[:, lanes] = low

    def dot_t(a, b):
        return lax.dot_general(
            a, b, (((1,), (1,)), ((), ())), preferred_element_type=jnp.float32
        )

    grad = (
        dot_t(r_high[...], h_high[...])
        + dot_t(r_high[...], h_low[...])
        + dot_t(r_low[...], h_high[...])
    ) * (scale / BATCH)
    for tap in range(TAPS):
        both[:, C * tap : C * (tap + 1)] = grad[PAIR * tap : PAIR * (tap + 1)]

    @pl.when(x == 0)
    def _():
        keep[...] = both[:OWN]
        send[...] = both[OWN:]

    @pl.when(x != 0)
    def _():
        keep[...] = both[OWN:]
        send[...] = both[:OWN]


def gradient(x_index, own_k, pair_k, own, gathered):
    operands = (x_index, own_k, pair_k, own[0], own[2], own[4], *gathered)
    flat = jax.ShapeDtypeStruct((OWN, KKC), jnp.float32)
    return pl.pallas_call(
        gradient_kernel,
        in_specs=[SMEM] + [VMEM] * (len(operands) - 1),
        out_specs=[VMEM, VMEM],
        out_shape=[flat, flat],
        scratch_shapes=[
            pltpu.VMEM((PAIR, KKC), jnp.float32),
            pltpu.VMEM((TAPS * PAIR, C), jnp.float32),
            pltpu.VMEM((TAPS * PAIR, PIX), jnp.float32),
            pltpu.VMEM((C, Z * PIX), jnp.bfloat16),
            pltpu.VMEM((C, Z * PIX), jnp.bfloat16),
            pltpu.VMEM((TAPS * PAIR, Z * PIX), jnp.bfloat16),
            pltpu.VMEM((TAPS * PAIR, Z * PIX), jnp.bfloat16),
        ],
        cost_estimate=pl.CostEstimate(
            flops=3_000_000_000, bytes_accessed=5_000_000, transcendentals=0
        ),
        name="gradient",
    )(*operands)


def shift(value, axis, steps):
    count = lax.axis_size(axis)
    return lax.ppermute(value, axis, [(i, (i + steps) % count) for i in range(count)])


def gather(parts):
    up0, dn0, up1, dn1 = parts[:4]
    got = [[], [], [], []]
    for hop in (1, 2, 3, 4):
        up0 = shift(up0, "z", 1)
        got[0].append(up0)
        if hop < 4:
            dn0 = shift(dn0, "z", -1)
            got[1].append(dn0)
            up1 = shift(up1, "z", 1)
            got[2].append(up1)
        dn1 = shift(dn1, "z", -1)
        got[3].append(dn1)
    return tuple(got[0] + got[1] + got[2] + got[3])


def local(
    latents, gaussian, stamps, numerator, momentum, push_weight, arrived_numerator, arrived_weight
):
    z_index = lax.axis_index("z").astype(jnp.int32)[None]
    x_index = lax.axis_index("x").astype(jnp.int32)[None]
    table = jnp.asarray(level_table())
    numerator, momentum, arrived_numerator = numerator[0], momentum[0], arrived_numerator[0]

    weight_1 = 0.5 * push_weight + arrived_weight
    arrived_weight_1 = shift(0.5 * push_weight, "rep", 1)
    weight_out = 0.5 * weight_1 + arrived_weight_1
    pending_weight = shift(0.5 * weight_1, "rep", 2)

    own = [prepare(k, z_index, stamps, table, latents, gaussian) for k in range(STEPS)]
    first = gather(own[0])
    first, own[1] = lax.optimization_barrier((first, own[1]))
    second = gather(own[1])
    weights = (push_weight, weight_1)
    kernel = numerator / push_weight
    for k in range(STEPS):
        keep, send = gradient(
            x_index, kernel, shift(kernel, "x", 1), own[k], first if k == 0 else second
        )
        momentum = momentum_decay * momentum + (keep + shift(send, "x", 1))
        moved = numerator - step_size * momentum
        half = 0.5 * moved
        numerator = half + arrived_numerator
        arrived_numerator = shift(half, "rep", 2**k)
        if k == 0:
            kernel = numerator / weights[1]
    return (
        numerator[None],
        momentum[None],
        weight_out,
        arrived_numerator[None],
        pending_weight,
    )


def solution(mesh):
    split = Mesh(mesh.devices.reshape(mesh.shape["rep"], Z, 2), ("rep", "z", "x"))
    fsdp = ("z", "x")
    every = ("rep", "z", "x")
    state = P("rep", fsdp, None)
    return jax.shard_map(
        local,
        mesh=split,
        in_specs=(
            P(None, every, None, None),
            P(None, every, None, None),
            P(None, every),
            state,
            state,
            P("rep"),
            state,
            P("rep"),
        ),
        out_specs=(state, state, P("rep"), state, P("rep")),
        check_vma=False,
    )
```

```python
import functools

import numpy as np
import jax
import jax.numpy as jnp
from jax import lax
from jax.experimental import pallas as pl
from jax.experimental.pallas import tpu as pltpu
from jax.sharding import Mesh
from jax.sharding import PartitionSpec as P


C = 320
GROUP = 10
SIDE = 16
PIX = 256
TAPS = 9
STEPS = 2
TRAIN_T = 1000
KKC = 2880
Z = 8
OWN = 20
PAIR = 40
HALF = 160
BATCH = 16
ROWS = 368

norm_epsilon = 1e-05
momentum_decay = 0.9
step_size = 1.0
beta_first = 0.00085
beta_last = 0.012

VMEM = pl.BlockSpec(memory_space=pltpu.VMEM)
SMEM = pl.BlockSpec(memory_space=pltpu.SMEM)


def level_table():
    fraction = np.arange(TRAIN_T, dtype=np.float64) / (TRAIN_T - 1)
    first, last = beta_first**0.5, beta_last**0.5
    levels = np.cumprod(1.0 - np.square(first + fraction * (last - first)))
    table = np.zeros(1024, np.float32)
    table[:TRAIN_T] = levels.astype(np.float32)
    return table.reshape(8, 128)


def tap_offset(tap):
    return (tap // 3 - 1, tap % 3 - 1)


def tap_mask(tap, rows):
    pixel = lax.broadcasted_iota(jnp.int32, (rows, PIX), 1)
    row, column = pixel >> 4, pixel & 15
    down, right = tap_offset(tap)
    ok = None
    if down:
        ok = (row + down >= 0) & (row + down < SIDE)
    if right:
        side = (column + right >= 0) & (column + right < SIDE)
        ok = side if ok is None else ok & side
    return ok


def split_bf16(value):
    high = value.astype(jnp.bfloat16)
    low = (value - high.astype(jnp.float32)).astype(jnp.bfloat16)
    return high, low


def prepare_kernel(
    step, z_ref, stamps_ref, table_ref, lat, gau, up0, dn0, up1, dn1, own_t, gap, lat_ref, gau_ref, arrived
):
    fetch = [
        pltpu.make_async_copy(source.at[step, 0], target, arrived.at[index])
        for index, (source, target) in enumerate(((lat, lat_ref), (gau, gau_ref)))
    ]
    for copy in fetch:
        copy.start()
    stamp = stamps_ref[step]
    spot = lax.broadcasted_iota(jnp.int32, (8, 128), 0) * 128 + lax.broadcasted_iota(
        jnp.int32, (8, 128), 1
    )
    level = jnp.sum(jnp.where(spot == stamp, table_ref[...], 0.0), axis=(0, 1), keepdims=True)
    row_group = (lax.broadcasted_iota(jnp.int32, (C, C), 0) * 205) >> 11
    col_group = (lax.broadcasted_iota(jnp.int32, (C, C), 1) * 205) >> 11
    same = jnp.where(row_group == col_group, 1.0, 0.0).astype(jnp.float32)

    for copy in fetch:
        copy.wait()
    gaussian = gau_ref[...]
    noised = jnp.sqrt(level) * lat_ref[...] + jnp.sqrt(1.0 - level) * gaussian
    gap[...] = noised - gaussian

    def group_mean(value):
        sums = jnp.broadcast_to(jnp.sum(value, axis=1, keepdims=True), (C, 128))
        mixed = jnp.dot(
            same, sums, precision=lax.Precision.HIGHEST, preferred_element_type=jnp.float32
        )
        return mixed[:, :1] * (1.0 / (GROUP * PIX))

    centered = noised - group_mean(noised)
    normed = centered * lax.rsqrt(group_mean(centered * centered) + norm_epsilon)
    hidden = normed / (1.0 + jnp.exp(-normed))
    up0[:HALF] = hidden[:HALF]
    dn0[:HALF] = hidden[:HALF]
    up1[:HALF] = hidden[HALF:]
    dn1[:HALF] = hidden[HALF:]

    z = z_ref[0]

    def rows_of(distance, start, count):
        first = lax.rem(z + distance + Z, Z) * PAIR + start
        return gap[pl.ds(pl.multiple_of(first, 8), count), :]

    for hop in (1, 2, 3):
        at = HALF + PAIR * (hop - 1)
        up1[at : at + PAIR] = rows_of(hop, 0, PAIR)
        dn0[at : at + PAIR] = rows_of(-hop, 0, PAIR)
    up0[HALF : HALF + 24] = rows_of(4, 0, 24)
    dn1[HALF : HALF + 16] = rows_of(4, 24, 16)
    own_t[...] = rows_of(0, 0, PAIR)


def prepare(step, z_index, stamps, table, latents, gaussian):
    sizes = (HALF + 24, HALF + 120, HALF + 120, HALF + 16, PAIR)
    inputs = pl.BlockSpec(memory_space=pltpu.HBM)
    block = pltpu.VMEM((C, PIX), jnp.float32)
    return pl.pallas_call(
        functools.partial(prepare_kernel, step),
        in_specs=[SMEM, SMEM, VMEM, inputs, inputs],
        out_specs=[VMEM] * len(sizes),
        out_shape=[jax.ShapeDtypeStruct((rows, PIX), jnp.float32) for rows in sizes],
        scratch_shapes=[block, block, block, pltpu.SemaphoreType.DMA((2,))],
        cost_estimate=pl.CostEstimate(
            flops=200_000_000, bytes_accessed=2_000_000, transcendentals=82_000
        ),
        compiler_params=pltpu.CompilerParams(vmem_limit_bytes=16 * 1024 * 1024),
        name="prepare",
    )(z_index, stamps, table, latents, gaussian)


def gradient_kernel(first, x_ref, *refs):
    if first:
        (own_k, pair_k), refs = refs[:2], refs[2:]
    else:
        (k_split, carried), refs = refs[:2], refs[2:]
    count = 6 if first else 2
    if first:
        buffers, refs = refs[:12], refs[12:]
        (total, k_split), refs = refs[:2], refs[2:]
    else:
        buffers, refs = refs[:5], refs[5:]
        (keep, send), refs = refs[:2], refs[2:]
    h_high, h_low, gaps, shifted, grad = refs
    x = x_ref[0]
    scale = KKC**-0.5
    shifted[...] = jnp.zeros_like(shifted)

    if first:
        grad[TAPS * PAIR :] = jnp.zeros((ROWS - TAPS * PAIR, C), jnp.float32)
        for tap in range(TAPS):
            lanes = slice(C * tap, C * (tap + 1))
            grad[PAIR * tap : PAIR * tap + OWN] = own_k[:, lanes]
            grad[PAIR * tap + OWN : PAIR * (tap + 1)] = pair_k[:, lanes]
        k_split[:ROWS], k_split[ROWS:] = split_bf16(grad[...])
        grad[...] = jnp.zeros_like(grad)
    else:
        grad[...] = carried[...]

    for index in range(count):
        if first:
            upper, lower = buffers[2 * index : 2 * index + 2]
            number, way = index // 2 + 1, index % 2
            start = HALF + PAIR * (number - 1)
            rows = (upper if way else lower)[start : start + PAIR]
        elif index == 0:
            upper, lower, gap = buffers[:3]
            rows = gap[...]
        else:
            upper, lower = buffers[3:]
            rows = jnp.concatenate([upper[HALF : HALF + 24], lower[HALF : HALF + 16]], axis=0)
        gaps[index // 2, index % 2] = jnp.where(
            x == 0, rows, jnp.concatenate([rows[OWN:], rows[:OWN]], axis=0)
        )
        for part, block in ((0, upper), (HALF, lower)):
            high, low = split_bf16(block[:HALF])
            h_high[index // 2, index % 2, part : part + HALF] = high
            h_low[index // 2, index % 2, part : part + HALF] = low

    def dot(a, b):
        return jnp.dot(a, b, preferred_element_type=jnp.float32)

    def dot_t(a, b):
        return lax.dot_general(a, b, (((1,), (1,)), ((), ())), preferred_element_type=jnp.float32)

    masks = [tap_mask(tap, PAIR) for tap in range(TAPS)]

    def one(index, side):
        high, low = h_high[index, side], h_low[index, side]
        both = dot(k_split[...], high)
        product = both[:ROWS] + both[ROWS:] + dot(k_split[:ROWS], low)
        output = product[4 * PAIR : 5 * PAIR]
        for tap in range(TAPS):
            if tap == 4:
                continue
            down, right = tap_offset(tap)
            moved = pltpu.roll(
                product[PAIR * tap : PAIR * (tap + 1)], (-(SIDE * down + right)) % PIX, 1
            )
            output = output + jnp.where(masks[tap], moved, 0.0)
        residual = gaps[index, side] + scale * output
        for tap in range(TAPS):
            down, right = tap_offset(tap)
            value = residual
            if tap != 4:
                value = pltpu.roll(
                    jnp.where(masks[tap], residual, 0.0), (SIDE * down + right) % PIX, 1
                )
            shifted[side, PAIR * tap : PAIR * (tap + 1)] = value
        r_high, r_low = split_bf16(shifted[side])
        both = dot_t(jnp.concatenate([r_high, r_low], axis=0), high)
        return both[:ROWS] + both[ROWS:] + dot_t(r_high, low)

    def pair(index):
        grad[...] += one(index, 0) + one(index, 1)

    if first:
        lax.fori_loop(0, count // 2, lambda index, _: (pair(index), 0)[1], 0)
        total[...] = grad[...]
    else:
        pair(0)
        for tap in range(TAPS):
            lanes = slice(C * tap, C * (tap + 1))
            result = grad[PAIR * tap : PAIR * (tap + 1)] * (scale / BATCH)
            keep[:, lanes] = result[:OWN]
            send[:, lanes] = result[OWN:]


def gradient(first, *operands):
    flat = jax.ShapeDtypeStruct((OWN, KKC), jnp.float32)
    total = jax.ShapeDtypeStruct((ROWS, C), jnp.float32)
    halves = jax.ShapeDtypeStruct((2 * ROWS, C), jnp.bfloat16)
    pairs = 3 if first else 1
    return pl.pallas_call(
        functools.partial(gradient_kernel, first),
        in_specs=[SMEM] + [VMEM] * (len(operands) - 1),
        out_specs=[VMEM, VMEM],
        out_shape=[total, halves] if first else [flat, flat],
        scratch_shapes=[
            pltpu.VMEM((pairs, 2, C, PIX), jnp.bfloat16),
            pltpu.VMEM((pairs, 2, C, PIX), jnp.bfloat16),
            pltpu.VMEM((pairs, 2, PAIR, PIX), jnp.float32),
            pltpu.VMEM((2, ROWS, PIX), jnp.float32),
            pltpu.VMEM((ROWS, C), jnp.float32),
        ],
        cost_estimate=pl.CostEstimate(
            flops=800_000_000 * pairs, bytes_accessed=1_200_000 * pairs, transcendentals=0
        ),
        compiler_params=pltpu.CompilerParams(vmem_limit_bytes=16 * 1024 * 1024),
        name="gradient",
    )(*operands)


def shift(value, axis, steps):
    count = lax.axis_size(axis)
    return lax.ppermute(value, axis, [(i, (i + steps) % count) for i in range(count)])


def hop(number, parts):
    names = ("up0", "dn0", "up1", "dn1")
    return tuple(
        shift(part, "z", 1 if name[0] == "u" else -1)
        if number < 4 or name in ("up0", "dn1")
        else None
        for part, name in zip(parts, names)
    )


def early(x_index, kernel, hops):
    buffers = []
    for got in hops:
        buffers += [got[0], got[2], got[1], got[3]]
    pair = shift(kernel, "x", 1)
    return gradient(True, x_index, kernel, pair, *buffers)


def late(x_index, state, own, four):
    total, k_split = state
    keep, send = gradient(False, x_index, k_split, total, own[0], own[2], own[4], four[0], four[3])
    return keep, shift(send, "x", 1)


def update(numerator, momentum, arrived, keep, received):
    momentum = momentum_decay * momentum + (keep + received)
    half = 0.5 * (numerator - step_size * momentum)
    return half, momentum, half + arrived


def send_on(half, weight, steps):
    message = lax.pad(half, weight[0], ((0, 1, 0), (0, 0, 0)))
    message = shift(message, "rep", steps)
    return message[:OWN], message[OWN, :1]


def both_steps(
    latents, gaussian, stamps, numerator, momentum, push_weight, arrived_numerator, arrived_weight
):
    z_index = lax.axis_index("z").astype(jnp.int32)[None]
    x_index = lax.axis_index("x").astype(jnp.int32)[None]
    table = jnp.asarray(level_table())
    stamps = stamps.reshape(STEPS)
    numerator, momentum, arrived_numerator = numerator[0], momentum[0], arrived_numerator[0]
    weight_1 = 0.5 * push_weight + arrived_weight

    own = prepare(0, z_index, stamps, table, latents, gaussian)
    kernel = numerator / push_weight
    one = hop(1, own[:4])
    next_own = prepare(1, z_index, stamps, table, latents, gaussian)
    two = hop(2, one)
    three = hop(3, two)
    state = early(x_index, kernel, (one, two, three))
    three, next_own = lax.optimization_barrier((three, next_own))
    four = hop(4, three)
    next_one = hop(1, next_own[:4])
    keep, received = late(x_index, state, own, four)
    half, momentum, numerator = update(numerator, momentum, arrived_numerator, keep, received)
    kernel = numerator / weight_1
    arrived_numerator, arrived_weight = send_on(half, 0.5 * push_weight, 1)

    next_two = hop(2, next_one)
    next_three = hop(3, next_two)
    next_four = hop(4, next_three)
    state = early(x_index, kernel, (next_one, next_two, next_three))
    keep, received = late(x_index, state, next_own, next_four)
    half, momentum, numerator = update(numerator, momentum, arrived_numerator, keep, received)
    pending, pending_weight = send_on(half, 0.5 * weight_1, 2)
    return (
        numerator[None],
        momentum[None],
        0.5 * weight_1 + arrived_weight,
        pending[None],
        pending_weight,
    )


def solution(mesh):
    split = Mesh(mesh.devices.reshape(mesh.shape["rep"], Z, 2), ("rep", "z", "x"))
    fsdp = ("z", "x")
    every = ("rep", "z", "x")
    state = P("rep", fsdp, None)
    return jax.shard_map(
        both_steps,
        mesh=split,
        in_specs=(
            P(None, every, None, None),
            P(None, every, None, None),
            P(None, every),
            state,
            state,
            P("rep"),
            state,
            P("rep"),
        ),
        out_specs=(state, state, P("rep"), state, P("rep")),
        check_vma=False,
    )
```

```python
import functools

import numpy as np
import jax
import jax.numpy as jnp
from jax import lax
from jax.experimental import pallas as pl
from jax.experimental.pallas import tpu as pltpu
from jax.sharding import Mesh
from jax.sharding import PartitionSpec as P


C = 320
GROUP = 10
GROUPS = 32
SIDE = 16
PIX = 256
TAPS = 9
STEPS = 2
TRAIN_T = 1000
KKC = 2880
Z = 8
OWN = 20
PAIR = 40
HALF = 160
BATCH = 16
ROWS = 368

norm_epsilon = 1e-05
momentum_decay = 0.9
step_size = 1.0
beta_first = 0.00085
beta_last = 0.012

VMEM = pl.BlockSpec(memory_space=pltpu.VMEM)
SMEM = pl.BlockSpec(memory_space=pltpu.SMEM)


def level_table():
    fraction = np.arange(TRAIN_T, dtype=np.float64) / (TRAIN_T - 1)
    first, last = beta_first**0.5, beta_last**0.5
    levels = np.cumprod(1.0 - np.square(first + fraction * (last - first)))
    table = np.zeros(1024, np.float32)
    table[:TRAIN_T] = levels.astype(np.float32)
    return table.reshape(8, 128)


def tap_offset(tap):
    return (tap // 3 - 1, tap % 3 - 1)


def tap_mask(tap, rows):
    pixel = lax.broadcasted_iota(jnp.int32, (rows, PIX), 1)
    row, column = pixel >> 4, pixel & 15
    down, right = tap_offset(tap)
    ok = None
    if down:
        ok = (row + down >= 0) & (row + down < SIDE)
    if right:
        side = (column + right >= 0) & (column + right < SIDE)
        ok = side if ok is None else ok & side
    return ok


def split_bf16(value):
    high = value.astype(jnp.bfloat16)
    low = (value - high.astype(jnp.float32)).astype(jnp.bfloat16)
    return high, low


def prepare_kernel(
    step, z_ref, stamps_ref, table_ref, lat, gau, up0, dn0, up1, dn1, own_t, gap, lat_ref, gau_ref, arrived
):
    fetch = [
        pltpu.make_async_copy(source.at[step, 0], target, arrived.at[index])
        for index, (source, target) in enumerate(((lat, lat_ref), (gau, gau_ref)))
    ]
    for copy in fetch:
        copy.start()
    stamp = stamps_ref[step]
    spot = lax.broadcasted_iota(jnp.int32, (8, 128), 0) * 128 + lax.broadcasted_iota(
        jnp.int32, (8, 128), 1
    )
    level = jnp.sum(jnp.where(spot == stamp, table_ref[...], 0.0), axis=(0, 1), keepdims=True)

    def member(shape, axis):
        channel = lax.broadcasted_iota(jnp.int32, shape, axis)
        group = lax.broadcasted_iota(jnp.int32, shape, 1 - axis)
        return jnp.where((channel * 205) >> 11 == group, 1.0, 0.0).astype(jnp.float32)

    gather_groups, spread_groups = member((GROUPS, C), 1), member((C, GROUPS), 0)

    def mix(a, b):
        return jnp.dot(a, b, precision=lax.Precision.HIGHEST, preferred_element_type=jnp.float32)

    for copy in fetch:
        copy.wait()
    gaussian = gau_ref[...]
    noised = jnp.sqrt(level) * lat_ref[...] + jnp.sqrt(1.0 - level) * gaussian
    gap[...] = noised - gaussian

    def group_mean(value):
        sums = jnp.broadcast_to(jnp.sum(value, axis=1, keepdims=True), (C, 128))
        mixed = mix(spread_groups, mix(gather_groups, sums))
        return mixed[:, :1] * (1.0 / (GROUP * PIX))

    centered = noised - group_mean(noised)
    normed = centered * lax.rsqrt(group_mean(centered * centered) + norm_epsilon)
    hidden = normed / (1.0 + jnp.exp(-normed))
    up0[:HALF] = hidden[:HALF]
    dn0[:HALF] = hidden[:HALF]
    up1[:HALF] = hidden[HALF:]
    dn1[:HALF] = hidden[HALF:]

    z = z_ref[0]

    def rows_of(distance, start, count):
        first = lax.rem(z + distance + Z, Z) * PAIR + start
        return gap[pl.ds(pl.multiple_of(first, 8), count), :]

    for hop in (1, 2, 3):
        at = HALF + PAIR * (hop - 1)
        up1[at : at + PAIR] = rows_of(hop, 0, PAIR)
        dn0[at : at + PAIR] = rows_of(-hop, 0, PAIR)
    up0[HALF : HALF + 24] = rows_of(4, 0, 24)
    dn1[HALF : HALF + 16] = rows_of(4, 24, 16)
    own_t[...] = rows_of(0, 0, PAIR)


def prepare(step, z_index, stamps, table, latents, gaussian):
    sizes = (HALF + 24, HALF + 120, HALF + 120, HALF + 16, PAIR)
    inputs = pl.BlockSpec(memory_space=pltpu.HBM)
    block = pltpu.VMEM((C, PIX), jnp.float32)
    return pl.pallas_call(
        functools.partial(prepare_kernel, step),
        in_specs=[SMEM, SMEM, VMEM, inputs, inputs],
        out_specs=[VMEM] * len(sizes),
        out_shape=[jax.ShapeDtypeStruct((rows, PIX), jnp.float32) for rows in sizes],
        scratch_shapes=[block, block, block, pltpu.SemaphoreType.DMA((2,))],
        cost_estimate=pl.CostEstimate(
            flops=200_000_000, bytes_accessed=2_000_000, transcendentals=82_000
        ),
        compiler_params=pltpu.CompilerParams(vmem_limit_bytes=16 * 1024 * 1024),
        name="prepare",
    )(z_index, stamps, table, latents, gaussian)


def gradient_kernel(first, joined, x_ref, *refs):
    if first:
        if joined:
            own_k, pair_k, refs = refs[0].at[0], refs[0].at[1], refs[1:]
        else:
            own_k, pair_k, refs = refs[0].at[0], refs[1].at[0], refs[2:]
    else:
        (k_split, carried), refs = refs[:2], refs[2:]
    count = 6 if first else 2
    if first:
        buffers, refs = refs[:12], refs[12:]
        (total, k_split), refs = refs[:2], refs[2:]
    else:
        buffers, refs = refs[:5], refs[5:]
        if joined:
            keep, send, refs = refs[0].at[0], refs[0].at[1], refs[1:]
        else:
            (keep, send), refs = refs[:2], refs[2:]
    h_high, h_low, gaps, shifted, grad = refs
    x = x_ref[0]
    scale = KKC**-0.5
    shifted[...] = jnp.zeros_like(shifted)

    if first:
        grad[TAPS * PAIR :] = jnp.zeros((ROWS - TAPS * PAIR, C), jnp.float32)
        for tap in range(TAPS):
            lanes = slice(C * tap, C * (tap + 1))
            grad[PAIR * tap : PAIR * tap + OWN] = own_k[:, lanes]
            grad[PAIR * tap + OWN : PAIR * (tap + 1)] = pair_k[:, lanes]
        k_split[:ROWS], k_split[ROWS:] = split_bf16(grad[...])
        grad[...] = jnp.zeros_like(grad)
    else:
        grad[...] = carried[...]

    for index in range(count):
        if first:
            upper, lower = buffers[2 * index : 2 * index + 2]
            number, way = index // 2 + 1, index % 2
            start = HALF + PAIR * (number - 1)
            rows = (upper if way else lower)[start : start + PAIR]
        elif index == 0:
            upper, lower, gap = buffers[:3]
            rows = gap[...]
        else:
            upper, lower = buffers[3:]
            rows = jnp.concatenate([upper[HALF : HALF + 24], lower[HALF : HALF + 16]], axis=0)
        gaps[index // 2, index % 2] = jnp.where(
            x == 0, rows, jnp.concatenate([rows[OWN:], rows[:OWN]], axis=0)
        )
        for part, block in ((0, upper), (HALF, lower)):
            high, low = split_bf16(block[:HALF])
            h_high[index // 2, index % 2, part : part + HALF] = high
            h_low[index // 2, index % 2, part : part + HALF] = low

    def dot(a, b):
        return jnp.dot(a, b, preferred_element_type=jnp.float32)

    def dot_t(a, b):
        return lax.dot_general(a, b, (((1,), (1,)), ((), ())), preferred_element_type=jnp.float32)

    masks = [tap_mask(tap, PAIR) for tap in range(TAPS)]

    def one(index, side):
        high, low = h_high[index, side], h_low[index, side]
        both = dot(k_split[...], high)
        product = both[:ROWS] + both[ROWS:] + dot(k_split[:ROWS], low)
        output = product[4 * PAIR : 5 * PAIR]
        for tap in range(TAPS):
            if tap == 4:
                continue
            down, right = tap_offset(tap)
            moved = pltpu.roll(
                product[PAIR * tap : PAIR * (tap + 1)], (-(SIDE * down + right)) % PIX, 1
            )
            output = output + jnp.where(masks[tap], moved, 0.0)
        residual = gaps[index, side] + scale * output
        for tap in range(TAPS):
            down, right = tap_offset(tap)
            value = residual
            if tap != 4:
                value = pltpu.roll(
                    jnp.where(masks[tap], residual, 0.0), (SIDE * down + right) % PIX, 1
                )
            shifted[side, PAIR * tap : PAIR * (tap + 1)] = value
        r_high, r_low = split_bf16(shifted[side])
        both = dot_t(jnp.concatenate([r_high, r_low], axis=0), high)
        return both[:ROWS] + both[ROWS:] + dot_t(r_high, low)

    def pair(index):
        grad[...] += one(index, 0) + one(index, 1)

    if first:
        lax.fori_loop(0, count // 2, lambda index, _: (pair(index), 0)[1], 0)
        total[...] = grad[...]
    else:
        pair(0)
        for tap in range(TAPS):
            lanes = slice(C * tap, C * (tap + 1))
            result = grad[PAIR * tap : PAIR * (tap + 1)] * (scale / BATCH)
            keep[:, lanes] = result[:OWN]
            send[:, lanes] = result[OWN:]


def gradient(first, joined, *operands):
    flat = jax.ShapeDtypeStruct((OWN, KKC), jnp.float32)
    total = jax.ShapeDtypeStruct((ROWS, C), jnp.float32)
    halves = jax.ShapeDtypeStruct((2 * ROWS, C), jnp.bfloat16)
    if first:
        shapes = [total, halves]
    else:
        shapes = [jax.ShapeDtypeStruct((2, OWN, KKC), jnp.float32)] if joined else [flat, flat]
    pairs = 3 if first else 1
    return pl.pallas_call(
        functools.partial(gradient_kernel, first, joined),
        in_specs=[SMEM] + [VMEM] * (len(operands) - 1),
        out_specs=[VMEM] * len(shapes),
        out_shape=shapes,
        scratch_shapes=[
            pltpu.VMEM((pairs, 2, C, PIX), jnp.bfloat16),
            pltpu.VMEM((pairs, 2, C, PIX), jnp.bfloat16),
            pltpu.VMEM((pairs, 2, PAIR, PIX), jnp.float32),
            pltpu.VMEM((2, ROWS, PIX), jnp.float32),
            pltpu.VMEM((ROWS, C), jnp.float32),
        ],
        cost_estimate=pl.CostEstimate(
            flops=800_000_000 * pairs, bytes_accessed=1_200_000 * pairs, transcendentals=0
        ),
        compiler_params=pltpu.CompilerParams(vmem_limit_bytes=16 * 1024 * 1024),
        name="gradient",
    )(*operands)


def shift(value, axis, steps):
    count = lax.axis_size(axis)
    return lax.ppermute(value, axis, [(i, (i + steps) % count) for i in range(count)])


def hop(number, parts):
    names = ("up0", "dn0", "up1", "dn1")
    return tuple(
        shift(part, "z", 1 if name[0] == "u" else -1)
        if number < 4 or name in ("up0", "dn1")
        else None
        for part, name in zip(parts, names)
    )


def step_kernel(weight, mine, pair, both, received, kernels, grad):
    own, other = both[0] + received[1], both[1] + received[0]
    grad[...] = own
    kernels[0] = (mine[1] - 0.5 * step_size * own) / weight[0]
    kernels[1] = (pair[1] - 0.5 * step_size * other) / weight[0]


def next_kernels(weight, mine, pair, both, received):
    flat = jax.ShapeDtypeStruct((OWN, KKC), jnp.float32)
    two = jax.ShapeDtypeStruct((2, OWN, KKC), jnp.float32)
    return pl.pallas_call(
        step_kernel,
        in_specs=[SMEM] + [VMEM] * 4,
        out_specs=[VMEM, VMEM],
        out_shape=[two, flat],
        cost_estimate=pl.CostEstimate(flops=1_000_000, bytes_accessed=2_000_000, transcendentals=0),
        compiler_params=pltpu.CompilerParams(vmem_limit_bytes=16 * 1024 * 1024),
        name="next_kernels",
    )(weight, mine, pair, both, received)


def early(x_index, kernels, hops):
    buffers = []
    for got in hops:
        buffers += [got[0], got[2], got[1], got[3]]
    return gradient(True, len(kernels) == 1, x_index, *kernels, *buffers)


def late(joined, x_index, state, own, four):
    total, k_split = state
    return gradient(
        False, joined, x_index, k_split, total, own[0], own[2], own[4], four[0], four[3]
    )


def send_on(half, weight, steps):
    message = lax.pad(half, weight[0], ((0, 1, 0), (0, 0, 0)))
    message = shift(message, "rep", steps)
    return message[:OWN], message[OWN, :1]


def both_steps(
    latents, gaussian, stamps, numerator, momentum, push_weight, arrived_numerator, arrived_weight
):
    z_index = lax.axis_index("z").astype(jnp.int32)[None]
    x_index = lax.axis_index("x").astype(jnp.int32)[None]
    table = jnp.asarray(level_table())
    stamps = stamps.reshape(STEPS)
    numerator, momentum, arrived_numerator = numerator[0], momentum[0], arrived_numerator[0]
    weight_1 = 0.5 * push_weight + arrived_weight

    own = prepare(0, z_index, stamps, table, latents, gaussian)
    one = hop(1, own[:4])
    base = 0.5 * (numerator - step_size * momentum_decay * momentum) + arrived_numerator
    mine = jnp.stack([numerator / push_weight, base])
    next_own = prepare(1, z_index, stamps, table, latents, gaussian)
    one, mine = lax.optimization_barrier((one, mine))
    pair = shift(mine, "x", 1)
    two = hop(2, one)
    three = hop(3, two)
    state = early(x_index, (mine, pair), (one, two, three))
    three, next_own = lax.optimization_barrier((three, next_own))
    four = hop(4, three)
    next_one = hop(1, next_own[:4])
    (both,) = late(True, x_index, state, own, four)
    kernels, grad = next_kernels(weight_1, mine, pair, both, shift(both, "x", 1))

    next_two = hop(2, next_one)
    next_three = hop(3, next_two)
    next_four = hop(4, next_three)
    state = early(x_index, (kernels,), (next_one, next_two, next_three))
    keep, send = late(False, x_index, state, next_own, next_four)
    grad, keep, send = lax.optimization_barrier((grad, keep, send))
    received = shift(send, "x", 1)

    momentum = momentum_decay * momentum + grad
    half = 0.5 * (numerator - step_size * momentum)
    numerator = half + arrived_numerator
    arrived_numerator, arrived_weight = send_on(half, 0.5 * push_weight, 1)

    momentum = momentum_decay * momentum + (keep + received)
    half = 0.5 * (numerator - step_size * momentum)
    pending, pending_weight = send_on(half, 0.5 * weight_1, 2)
    return (
        (half + arrived_numerator)[None],
        momentum[None],
        0.5 * weight_1 + arrived_weight,
        pending[None],
        pending_weight,
    )


def solution(mesh):
    split = Mesh(mesh.devices.reshape(mesh.shape["rep"], Z, 2), ("rep", "z", "x"))
    fsdp = ("z", "x")
    every = ("rep", "z", "x")
    state = P("rep", fsdp, None)
    return jax.shard_map(
        both_steps,
        mesh=split,
        in_specs=(
            P(None, every, None, None),
            P(None, every, None, None),
            P(None, every),
            state,
            state,
            P("rep"),
            state,
            P("rep"),
        ),
        out_specs=(state, state, P("rep"), state, P("rep")),
        check_vma=False,
    )
```
